256 devices in a mesh: grp: 4 (over y), seq: 64 (over x, z, core).
Axes of the slice: x: 4, y: 4, z: 8, core: 2. Of those that a mesh axis runs over, the one named last changes fastest.
Arguments:
- queries: bfloat16 [65536, 2048], P(('grp', 'seq')), may hold values from -48 to 48
- key_rows: bfloat16 [65536, 512], P(('grp', 'seq')), may hold values from -4.5 to 4.5
- value_rows: bfloat16 [65536, 512], P(('grp', 'seq')), may hold values from -6 to 6
- segments: int32 [65536], P(('grp', 'seq')), may hold values from 0 to 30, as said below
Outputs:
- attended: bfloat16 [65536, 2048], P(('grp', 'seq'))
- log_sums: float32 [16, 65536], P(None, ('grp', 'seq'))
The draws below stay inside these ranges and needn't reach their ends.
Inputs may be any that keep to these rules, and one draw needn't show every extreme that they name: `segments`: never falls along the sequence, starts at 0 and rises by one at each new document; the last token holds the largest value.
All inputs are finite; a program needn't handle non-finite values.
Results may differ from the reference program's by a relative error of at most 0.0035.
Values may be sent and summed in bfloat16 or wider, within the bound.
A program may use at most 192 MiB of HBM per device.

```python
import math
import jax
import jax.numpy as jnp
from jax import lax

Q_HEADS = 16
KV_HEADS = 4
HEAD_DIM = 128
WINDOW = 4096
TOK_DEV = 256
SEQ_LEN = 65536


def boundary_flags(key):
    stretch = max(WINDOW // 2, 2)
    pieces = SEQ_LEN // stretch
    offsets = jax.random.randint(jax.random.fold_in(key, 11), (pieces,), 1, stretch)
    spots = jnp.arange(SEQ_LEN)
    first_mark = SEQ_LEN // 2 - TOK_DEV // 2
    second_mark = SEQ_LEN // 2 + TOK_DEV // 2
    low_piece = first_mark // stretch
    high_piece = min(pieces - 1, (second_mark + WINDOW) // stretch)
    piece_of = spots // stretch
    kept = (piece_of < low_piece) | (piece_of > high_piece)
    flags = (kept & (spots % stretch == offsets[piece_of])).astype(jnp.int32)
    flags = jnp.where((spots == first_mark) | (spots == second_mark), 1, flags)
    return flags.at[0].set(0)


def draw_segments(key, part):
    return jnp.cumsum(boundary_flags(key)).astype(jnp.int32)


def query_key_pair(key):
    group = Q_HEADS // KV_HEADS
    keys = jnp.clip(jax.random.normal(jax.random.fold_in(key, 21), (SEQ_LEN, KV_HEADS, HEAD_DIM), jnp.float32), -4.5, 4.5)
    queries = jnp.clip(3.0 * jax.random.normal(jax.random.fold_in(key, 22), (SEQ_LEN, KV_HEADS, group, HEAD_DIM), jnp.float32), -18.0, 18.0)
    return (queries.reshape(SEQ_LEN, Q_HEADS * HEAD_DIM).astype(jnp.bfloat16), keys.reshape(SEQ_LEN, KV_HEADS * HEAD_DIM).astype(jnp.bfloat16))


def draw_queries(key, part):
    return query_key_pair(key)[0]


def draw_key_rows(key, part):
    return query_key_pair(key)[1]


def steps_of(rng, extent, split, least, top_value):
    gain, own = 1.0, jax.random.fold_in(rng, 6)
    for position, blocks in split:
        heights = jnp.exp(jax.random.uniform(jax.random.fold_in(own, position), (blocks,), jnp.float32, least / len(split), top_value / len(split)))
        gain = gain * jnp.repeat(heights, extent[position] // blocks).reshape([-1 if axis == position else 1 for axis in range(len(extent))])
    return gain


def centred(key, dims, deviation, bound, cuts=(), kind=jnp.bfloat16):
    entries = jax.random.normal(key, dims, jnp.float32) * deviation
    if len(cuts) > 0:
        entries = steps_of(key, dims, cuts, -0.22, 0.18) * entries
    return jnp.clip(entries, min=-bound, max=bound).astype(kind)


def setup_inputs(seed: int = 0) -> dict:
    splits = jax.random.split(jax.random.key(seed), 5)
    return {
        "queries": draw_queries(jax.random.fold_in(splits[4], 71), 0),
        "key_rows": draw_key_rows(jax.random.fold_in(splits[4], 71), 0),
        "value_rows": centred(splits[2], (SEQ_LEN, KV_HEADS * HEAD_DIM), 1.0, 6.0, ((0, 256),)),
        "segments": draw_segments(jax.random.fold_in(splits[4], 71), 0),
    }


def reference(queries, key_rows, value_rows, segments):
    group = Q_HEADS // KV_HEADS
    block = math.gcd(SEQ_LEN, 512)
    count = SEQ_LEN // block
    span = block + WINDOW
    scale = 1.0 / math.sqrt(HEAD_DIM)
    width = KV_HEADS * HEAD_DIM
    key_pad = jnp.concatenate([jnp.zeros((WINDOW, width), key_rows.dtype), key_rows], axis=0)
    value_pad = jnp.concatenate([jnp.zeros((WINDOW, width), value_rows.dtype), value_rows], axis=0)
    seg_pad = jnp.concatenate([jnp.full((WINDOW,), -1, jnp.int32), segments.astype(jnp.int32)], axis=0)

    def one_block(index):
        first = (index * block).astype(jnp.int32)
        q_part = lax.dynamic_slice_in_dim(queries, first, block, 0).reshape(block, KV_HEADS, group, HEAD_DIM).astype(jnp.float32)
        k_part = lax.dynamic_slice_in_dim(key_pad, first, span, 0).reshape(span, KV_HEADS, HEAD_DIM).astype(jnp.float32)
        v_part = lax.dynamic_slice_in_dim(value_pad, first, span, 0).reshape(span, KV_HEADS, HEAD_DIM).astype(jnp.float32)
        q_seg = lax.dynamic_slice_in_dim(segments.astype(jnp.int32), first, block, 0)
        k_seg = lax.dynamic_slice_in_dim(seg_pad, first, span, 0)
        q_pos = first + jnp.arange(block, dtype=jnp.int32)
        k_pos = first - WINDOW + jnp.arange(span, dtype=jnp.int32)
        allowed = (k_pos[None, :] <= q_pos[:, None]) & (k_pos[None, :] > q_pos[:, None] - WINDOW) & (k_seg[None, :] == q_seg[:, None])
        scores = jnp.einsum('tkgd,lkd->kgtl', q_part, k_part, precision=lax.Precision.HIGHEST) * scale
        masked = jnp.where(allowed, scores, -1e+30)
        top = lax.optimization_barrier(jnp.max(masked, axis=-1))
        expo = jnp.where(allowed, jnp.exp(masked - top[..., None]), 0.0)
        total = lax.optimization_barrier(jnp.sum(expo, axis=-1))
        weights = lax.optimization_barrier(expo.astype(jnp.bfloat16))
        summed = jnp.einsum('kgtl,lkd->tkgd', weights.astype(jnp.float32), v_part, precision=lax.Precision.HIGHEST)
        out = summed / jnp.transpose(total, (2, 0, 1))[..., None]
        out = out.reshape(block, Q_HEADS * HEAD_DIM).astype(jnp.bfloat16)
        sums = (top + jnp.log(total)).reshape(Q_HEADS, block)
        return (out, sums)
    outs, sums = lax.map(one_block, jnp.arange(count, dtype=jnp.int32))
    attended = outs.reshape(SEQ_LEN, Q_HEADS * HEAD_DIM)
    log_sums = jnp.transpose(sums, (1, 0, 2)).reshape(Q_HEADS, SEQ_LEN)
    return (attended, log_sums)
```

```python
import math

import jax
import jax.numpy as jnp
from jax import lax
from jax.experimental import pallas as pl
from jax.experimental.pallas import tpu as pltpu
from jax.sharding import Mesh
from jax.sharding import PartitionSpec as P

Q_HEADS = 16
KV_HEADS = 4
GROUP = Q_HEADS // KV_HEADS
HEAD_DIM = 128
WINDOW = 4096
TOK = 256
GRP_SEQ = ("grp", "seq_0", "seq_1", "seq_2")
NX, NZ = 4, 8
CHIPS = 128
REACH = WINDOW // (2 * TOK)
SLOTS = 2 * REACH + 1
FWD = 3
ONES = 16
NEG = -1e30
SCALE = 1.0 / math.sqrt(HEAD_DIM)
LOG2 = SCALE * math.log2(math.e)
MESH = pl.DeviceIdType.MESH


def kernel(q_hbm, k_hbm, v_hbm, seg_hbm, out_ref, lse_ref, kv, seg, qv, qt, acc, top, load_sem, recv_sem, send_sem, seg_recv, seg_send):
    y, x, z, core = (lax.axis_index(a) for a in GRP_SEQ)
    chip = (y * NX + x) * NZ + z

    def at(c, k):
        c = lax.rem(c + CHIPS, CHIPS)
        return (c // (NX * NZ), lax.rem(c // NZ, NX), lax.rem(c, NZ), k)

    ahead, behind = at(chip + 1, core), at(chip - 1, core)
    far, near = at(chip + REACH, core), at(chip - REACH, core)
    other = at(chip, 1 - core)

    loads = []
    for g in range(KV_HEADS):
        cols = pl.ds(g * HEAD_DIM, HEAD_DIM)
        loads.append(pltpu.make_async_copy(k_hbm.at[:, cols], kv.at[0, g, 0], load_sem.at[2 * g]))
        loads.append(pltpu.make_async_copy(v_hbm.at[:, cols], kv.at[0, g, 1], load_sem.at[2 * g + 1]))
    load_seg = pltpu.make_async_copy(seg_hbm, seg.at[0], load_sem.at[2 * KV_HEADS])
    load_q = pltpu.make_async_copy(q_hbm, qv, load_sem.at[2 * KV_HEADS + 1])
    load_seg.start()
    for copy in loads:
        copy.start()
    load_q.start()

    barrier = pltpu.get_barrier_semaphore()
    for peer in (ahead, behind, far, near, other):
        pl.semaphore_signal(barrier, inc=1, device_id=peer, device_id_type=MESH)
    pl.semaphore_wait(barrier, 5)

    def moved(src, g, dst, row, peer):
        return pltpu.make_async_remote_copy(
            src_ref=kv.at[src, g], dst_ref=kv.at[dst, g], send_sem=send_sem.at[row, g],
            recv_sem=recv_sem.at[dst, g], device_id=peer, device_id_type=MESH)

    def moved_seg(src, dst, row, peer):
        return pltpu.make_async_remote_copy(
            src_ref=seg.at[src], dst_ref=seg.at[dst], send_sem=seg_send.at[row],
            recv_sem=seg_recv.at[dst], device_id=peer, device_id_type=MESH)

    def send(src, g, dst, row, peer):
        @pl.when(g == 0)
        def _():
            moved_seg(src, dst, row, peer).start()

        moved(src, g, dst, row, peer).start()

    def arrive(slot, g):
        @pl.when(g == 0)
        def _():
            moved_seg(slot, slot, 0, other).wait_recv()

        moved(slot, g, slot, 0, other).wait_recv()

    def share(j, g):
        t = j - core
        send(j, g, REACH + 1 + t, 8 + t, other)

    load_seg.wait()
    for g in range(KV_HEADS):
        loads[2 * g].wait()
        loads[2 * g + 1].wait()
        send(0, g, REACH, 7, far)
        send(0, g, 1, 0, ahead)

        @pl.when(core == 0)
        def _():
            share(0, g)

    load_q.wait()

    def turn(h, carry):
        qt[h] = qv[:, pl.ds(pl.multiple_of(h * HEAD_DIM, HEAD_DIM), HEAD_DIM)].T
        return carry

    lax.fori_loop(0, Q_HEADS, turn, 0)

    mine = seg[0]
    mine_col = jnp.broadcast_to(mine.astype(jnp.float32), (HEAD_DIM, TOK)).T
    key_pos = lax.broadcasted_iota(jnp.int32, (TOK, TOK), 0)
    q_pos = lax.broadcasted_iota(jnp.int32, (TOK, TOK), 1)
    mine_col = jnp.concatenate([mine_col, mine_col], axis=1)
    diagonal = (mine_col == jnp.broadcast_to(mine.astype(jnp.float32), (TOK, TOK))) & (key_pos <= q_pos)
    q_row = lax.broadcasted_iota(jnp.int32, (1, TOK), 1)
    q_first = mine == mine[:, :1]

    def values_of(slot, g):
        ones = jnp.ones((ONES, TOK), jnp.bfloat16)
        return jnp.concatenate([kv[slot, g, 1].T, ones], axis=0)

    def scores_of(keys, h):
        return jnp.dot(keys, qt[h], preferred_element_type=jnp.float32)

    def own_block(g, carry):
        keys, values = kv[0, g, 0], values_of(0, g)
        for i in range(GROUP):
            h = g * GROUP + i
            s = jnp.where(diagonal, scores_of(keys, h), NEG)
            m = jnp.max(s, axis=0, keepdims=True)
            p = jnp.exp2(s * LOG2 - m * LOG2).astype(jnp.bfloat16)
            acc[h] = jnp.dot(values, p, preferred_element_type=jnp.float32)
            top[h] = m
        return carry

    lax.fori_loop(0, KV_HEADS, own_block, 0)

    def attend(slot, g):
        back = jnp.where(slot <= REACH, 2 * slot, 2 * (slot - REACH) - 1)
        before = jnp.sum(jnp.where(seg[slot] < mine[:, :1], 1.0, 0.0), axis=1, keepdims=True).astype(jnp.int32)
        lower = jnp.where(q_first, jnp.broadcast_to(before, (1, TOK)), TOK)
        lower = jnp.maximum(lower, jnp.where(back == 2 * REACH, q_row + 1, 0))
        lower = jnp.maximum(lower, jnp.where(2 * chip + core < back, TOK, 0))
        allowed = key_pos >= lower
        keys, values = kv[slot, g, 0], values_of(slot, g)
        for i in range(GROUP):
            h = g * GROUP + i
            s = jnp.where(allowed, scores_of(keys, h), NEG)
            old = top[h]
            m = jnp.maximum(old, jnp.max(s, axis=0, keepdims=True))
            p = jnp.exp2(s * LOG2 - m * LOG2).astype(jnp.bfloat16)
            update = jnp.dot(values, p, preferred_element_type=jnp.float32)
            acc[h] = acc[h] * jnp.exp2((old - m) * LOG2) + update
            top[h] = m

    def tick(t, carry):
        @pl.when(t < KV_HEADS)
        def _():
            arrive(REACH, t)
            send(REACH, t, REACH - 1, 3, behind)

            @pl.when(core == 1)
            def _():
                share(REACH, t)

        @pl.when(t < FWD * KV_HEADS)
        def _():
            j, g = 1 + t // KV_HEADS, lax.rem(t, KV_HEADS)
            arrive(j, g)

            @pl.when(j < FWD)
            def _():
                send(j, g, j + 1, j, ahead)

            share(j, g)

        @pl.when((t >= 1) & (t <= (REACH - 1 - FWD) * KV_HEADS))
        def _():
            b = t - 1
            j, g = REACH - 1 - b // KV_HEADS, lax.rem(b, KV_HEADS)
            arrive(j, g)

            @pl.when(j > FWD + 1)
            def _():
                send(j, g, j - 1, 3 + REACH - j, behind)

            share(j, g)

        def source(r, carry):
            late = lax.rem(r, 2)
            u = t - late
            kind = r // 2
            b = u - jnp.where(kind == 1, 1, 0)
            steps = jnp.where(kind == 0, FWD, jnp.where(kind == 1, REACH - 1 - FWD, 1)) * KV_HEADS
            valid = (b >= 0) & (b < steps)
            bb = jnp.maximum(b, 0)
            j = jnp.where(kind == 0, 1 + bb // KV_HEADS, jnp.where(kind == 1, REACH - 1 - bb // KV_HEADS, REACH))
            g = lax.rem(bb, KV_HEADS)
            paired = jnp.where(kind == 2, 2 * REACH - (REACH - 1) * core, REACH + j + core)
            slot = jnp.where(late == 1, paired, j)

            @pl.when(valid)
            def _():
                @pl.when(late == 1)
                def _():
                    arrive(slot, g)

                attend(slot, g)

            return carry

        lax.fori_loop(0, 6, source, 0)
        return carry

    lax.fori_loop(0, (REACH - 1 - FWD) * KV_HEADS + 2, tick, 0)

    def finish(h, carry):
        total = acc[h, HEAD_DIM:HEAD_DIM + 1, :]
        part = acc[h, :HEAD_DIM, :] / total
        out_ref[:, pl.ds(pl.multiple_of(h * HEAD_DIM, HEAD_DIM), HEAD_DIM)] = part.T.astype(jnp.bfloat16)
        lse_ref[pl.ds(h, 1), :] = top[h] * SCALE + jnp.log(total)
        return carry

    lax.fori_loop(0, Q_HEADS, finish, 0)

    def drain(i, carry):
        row = i // KV_HEADS
        g = lax.rem(i, KV_HEADS)
        moved(0, g, 1, row, other).wait_send()

        @pl.when(g == 0)
        def _():
            moved_seg(0, 1, row, other).wait_send()

        return carry

    lax.fori_loop(0, 16 * KV_HEADS, drain, 0)


def on_device(queries, key_rows, value_rows, segments):
    return pl.pallas_call(
        kernel,
        out_shape=(
            jax.ShapeDtypeStruct((TOK, Q_HEADS * HEAD_DIM), jnp.bfloat16),
            jax.ShapeDtypeStruct((Q_HEADS, TOK), jnp.float32),
        ),
        in_specs=[pl.BlockSpec(memory_space=pl.ANY)] * 4,
        out_specs=(pl.BlockSpec(memory_space=pltpu.VMEM), pl.BlockSpec(memory_space=pltpu.VMEM)),
        scratch_shapes=[
            pltpu.VMEM((SLOTS, KV_HEADS, 2, TOK, HEAD_DIM), jnp.bfloat16),
            pltpu.VMEM((SLOTS, 1, TOK), jnp.int32),
            pltpu.VMEM((TOK, Q_HEADS * HEAD_DIM), jnp.bfloat16),
            pltpu.VMEM((Q_HEADS, HEAD_DIM, TOK), jnp.bfloat16),
            pltpu.VMEM((Q_HEADS, HEAD_DIM + ONES, TOK), jnp.float32),
            pltpu.VMEM((Q_HEADS, 1, TOK), jnp.float32),
            pltpu.SemaphoreType.DMA((2 * KV_HEADS + 2,)),
            pltpu.SemaphoreType.DMA((SLOTS, KV_HEADS)),
            pltpu.SemaphoreType.DMA((16, KV_HEADS)),
            pltpu.SemaphoreType.DMA((SLOTS,)),
            pltpu.SemaphoreType.DMA((16,)),
        ],
        compiler_params=pltpu.CompilerParams(
            collective_id=0, has_side_effects=True, vmem_limit_bytes=60 * 1024 * 1024),
    )(queries, key_rows, value_rows, segments.reshape(1, TOK))


def solution(mesh):
    split = Mesh(mesh.devices.reshape(mesh.shape["grp"], NX, NZ, 2), GRP_SEQ)
    rows = P(GRP_SEQ, None)
    return jax.shard_map(
        on_device,
        mesh=split,
        in_specs=(rows, rows, rows, P(GRP_SEQ)),
        out_specs=(rows, P(None, GRP_SEQ)),
        check_vma=False,
    )
```

```python
import math

import jax
import jax.numpy as jnp
from jax import lax
from jax.experimental import pallas as pl
from jax.experimental.pallas import tpu as pltpu
from jax.sharding import Mesh
from jax.sharding import PartitionSpec as P

Q_HEADS = 16
KV_HEADS = 4
GROUP = Q_HEADS // KV_HEADS
HEAD_DIM = 128
WINDOW = 4096
TOK = 256
GRP_SEQ = ("grp", "seq_0", "seq_1", "seq_2")
NX, NZ = 4, 8
CHIPS = 128
REACH = WINDOW // (2 * TOK)
SLOTS = 2 * REACH + 1
FWD = 3
BACK = REACH - 1 - FWD
ONES = 16
NEG = -1e30
BIG = -(2.0**100)
SCALE = 1.0 / math.sqrt(HEAD_DIM)
LOG2 = SCALE * math.log2(math.e)
MESH = pl.DeviceIdType.MESH


def kernel(q_hbm, k_hbm, v_hbm, seg_hbm, out_ref, lse_ref, kv, seg, qv, qt, acc, top, load_sem, recv_sem, send_sem, seg_recv, seg_send):
    y, x, z, core = (lax.axis_index(a) for a in GRP_SEQ)
    chip = (y * NX + x) * NZ + z

    def at(c, k):
        c = lax.rem(c + CHIPS, CHIPS)
        return (c // (NX * NZ), lax.rem(c // NZ, NX), lax.rem(c, NZ), k)

    ahead, behind = at(chip + 1, core), at(chip - 1, core)
    far, near = at(chip + REACH, core), at(chip - REACH, core)
    other = at(chip, 1 - core)

    loads = []
    for g in range(KV_HEADS):
        cols = pl.ds(g * HEAD_DIM, HEAD_DIM)
        loads.append(pltpu.make_async_copy(k_hbm.at[:, cols], kv.at[0, g, 0], load_sem.at[2 * g]))
        loads.append(pltpu.make_async_copy(v_hbm.at[:, cols], kv.at[0, g, 1], load_sem.at[2 * g + 1]))
    load_seg = pltpu.make_async_copy(seg_hbm, seg.at[0], load_sem.at[2 * KV_HEADS])
    load_q = pltpu.make_async_copy(q_hbm, qv, load_sem.at[2 * KV_HEADS + 1])
    load_seg.start()
    for copy in loads:
        copy.start()
    load_q.start()

    barrier = pltpu.get_barrier_semaphore()
    for peer in (ahead, behind, far, near, other):
        pl.semaphore_signal(barrier, inc=1, device_id=peer, device_id_type=MESH)
    pl.semaphore_wait(barrier, 5)

    def moved(src, g, dst, row, peer):
        return pltpu.make_async_remote_copy(
            src_ref=kv.at[src, g], dst_ref=kv.at[dst, g], send_sem=send_sem.at[row, g],
            recv_sem=recv_sem.at[dst, g], device_id=peer, device_id_type=MESH)

    def moved_seg(src, dst, row, peer):
        return pltpu.make_async_remote_copy(
            src_ref=seg.at[src], dst_ref=seg.at[dst], send_sem=seg_send.at[row],
            recv_sem=seg_recv.at[dst], device_id=peer, device_id_type=MESH)

    def send(src, g, dst, row, peer):
        @pl.when(g == 0)
        def _():
            moved_seg(src, dst, row, peer).start()

        moved(src, g, dst, row, peer).start()

    def arrive(slot, g):
        @pl.when(g == 0)
        def _():
            moved_seg(slot, slot, 0, other).wait_recv()

        moved(slot, g, slot, 0, other).wait_recv()

    def share(j, g):
        t = j - core
        send(j, g, REACH + 1 + t, 8 + t, other)

    load_seg.wait()
    for g in range(KV_HEADS):
        loads[2 * g].wait()
        loads[2 * g + 1].wait()
        send(0, g, REACH, 7, far)

        @pl.when(z != NZ - 1)
        def _():
            send(0, g, 1, 0, ahead)

        @pl.when(core == 0)
        def _():
            share(0, g)

    load_q.wait()

    mine = seg[0]
    q_row = lax.broadcasted_iota(jnp.int32, (1, TOK), 1)
    q_first = mine == mine[:, :1]
    sub = lax.broadcasted_iota(jnp.int32, (HEAD_DIM, TOK), 0)
    marks = jnp.where(sub == 0, 1.0, jnp.where(sub == 1, jnp.where(q_first, 0.0, 1.0), 0.0)).astype(jnp.bfloat16)

    def turn(h, carry):
        g, i = h // GROUP, lax.rem(h, GROUP)
        qt[g, i, :HEAD_DIM] = qv[:, pl.ds(pl.multiple_of(h * HEAD_DIM, HEAD_DIM), HEAD_DIM)].T
        qt[g, i, HEAD_DIM:] = marks
        return carry

    mine_col = jnp.broadcast_to(mine.astype(jnp.float32), (HEAD_DIM, TOK)).T
    key_pos = lax.broadcasted_iota(jnp.int32, (TOK, TOK), 0)
    q_pos = lax.broadcasted_iota(jnp.int32, (TOK, TOK), 1)
    mine_col = jnp.concatenate([mine_col, mine_col], axis=1)
    diagonal = (mine_col == jnp.broadcast_to(mine.astype(jnp.float32), (TOK, TOK))) & (key_pos <= q_pos)
    lane = lax.broadcasted_iota(jnp.int32, (TOK, HEAD_DIM), 1)
    key_row = lax.broadcasted_iota(jnp.int32, (TOK, HEAD_DIM), 0)

    def values_of(slot, g):
        ones = jnp.ones((ONES, TOK), jnp.bfloat16)
        return jnp.concatenate([kv[slot, g, 1].T, ones], axis=0)

    def heads(slot, g, keys, query_rows, mask, fresh):
        values = values_of(slot, g)
        old = None if fresh else [top[g, i] for i in range(GROUP)]

        def scores_of(i):
            return jnp.dot(keys, qt[g, i, :query_rows], preferred_element_type=jnp.float32)

        after = scores_of(0)
        maxima, factors, updates = [], [], []
        for i in range(GROUP):
            s = after
            if i + 1 < GROUP:
                after = scores_of(i + 1)
            if mask is not None:
                s = jnp.where(mask(), s, NEG)
            m = jnp.max(s, axis=0, keepdims=True)
            if not fresh:
                m = jnp.maximum(old[i], m)
                factors.append(jnp.exp2((old[i] - m) * LOG2))
            p = jnp.exp2(s * LOG2 - m * LOG2).astype(jnp.bfloat16)
            update = jnp.dot(values, p, preferred_element_type=jnp.float32)
            if fresh:
                acc[g, i] = update
            else:
                acc[g, i] = acc[g, i] * factors[i] + update
            maxima.append(m)
        for i in range(GROUP):
            top[g, i] = maxima[i]

    def attend(slot, g, window):
        back = jnp.where(slot <= REACH, 2 * slot, 2 * (slot - REACH) - 1)
        before = jnp.sum(jnp.where(seg[slot] < mine[:, :1], 1.0, 0.0), axis=1, keepdims=True).astype(jnp.int32)
        before = jnp.maximum(before, jnp.where(2 * chip + core < back, TOK, 0))
        if window:
            lower = jnp.where(q_first, jnp.broadcast_to(before, (1, TOK)), TOK)
            lower = jnp.maximum(lower, q_row + 1)
            heads(slot, g, kv[slot, g, 0], HEAD_DIM, lambda: key_pos >= lower, False)
        else:
            closed = jnp.where(key_row < before, BIG, 0.0)
            marks = jnp.where(lane == 0, closed, jnp.where(lane == 1, BIG, 0.0)).astype(jnp.bfloat16)
            heads(slot, g, jnp.concatenate([kv[slot, g, 0], marks], axis=1), 2 * HEAD_DIM, None, False)

    lag = jnp.where(z == 0, 5, jnp.where(z == 1, 3, 2))

    def tick(t, carry):
        @pl.when(t < KV_HEADS)
        def _():
            arrive(REACH, t)
            send(REACH, t, REACH - 1, 3, behind)

            @pl.when(core == 1)
            def _():
                share(REACH, t)

        @pl.when((t == KV_HEADS - 1) & (z == NZ - 1))
        def _():
            for g in range(KV_HEADS):
                send(0, g, 1, 0, ahead)

        b = t - 1

        @pl.when((b >= 0) & (b < BACK * KV_HEADS))
        def _():
            j, g = REACH - 1 - b // KV_HEADS, lax.rem(b, KV_HEADS)
            arrive(j, g)

            @pl.when(j > FWD + 1)
            def _():
                send(j, g, j - 1, 3 + REACH - j, behind)

            share(j, g)

        f = t - lag

        @pl.when((f >= 0) & (f < FWD * KV_HEADS))
        def _():
            j, g = 1 + f // KV_HEADS, lax.rem(f, KV_HEADS)
            arrive(j, g)

            @pl.when(j < FWD)
            def _():
                send(j, g, j + 1, j, ahead)

            share(j, g)

        @pl.when(t < KV_HEADS)
        def _():
            lax.fori_loop(t * GROUP, (t + 1) * GROUP, turn, 0)
            heads(0, t, kv[0, t, 0], HEAD_DIM, lambda: diagonal, True)

        def source(r, carry):
            kind = r // 2
            late = jnp.where(kind == 2, 1, lax.rem(r, 2))
            u = t - late - jnp.where(kind == 0, lag, jnp.where(kind == 1, 1, KV_HEADS - 1))
            steps = jnp.where(kind == 0, FWD, jnp.where(kind == 1, BACK, 1)) * KV_HEADS
            v = jnp.maximum(u, 0)
            j = jnp.where(kind == 0, 1 + v // KV_HEADS, REACH - 1 - v // KV_HEADS)
            g = lax.rem(v, KV_HEADS)
            paired = jnp.where(kind == 2, 2 * REACH - (REACH - 1) * core, REACH + j + core)
            slot = jnp.where(late == 1, paired, j)

            @pl.when((u >= 0) & (u < steps))
            def _():
                @pl.when(late == 1)
                def _():
                    arrive(slot, g)

                attend(slot, g, False)

            return carry

        @pl.when((t >= KV_HEADS) & (t < 2 * KV_HEADS))
        def _():
            attend(REACH, t - KV_HEADS, True)

        lax.fori_loop(0, 5, source, 0)
        return carry

    lax.fori_loop(0, BACK * KV_HEADS + 2, tick, 0)

    def finish(h, carry):
        g, i = h // GROUP, lax.rem(h, GROUP)
        total = acc[g, i, HEAD_DIM:HEAD_DIM + 1, :]
        part = acc[g, i, :HEAD_DIM, :] / total
        out_ref[:, pl.ds(pl.multiple_of(h * HEAD_DIM, HEAD_DIM), HEAD_DIM)] = part.T.astype(jnp.bfloat16)
        lse_ref[pl.ds(h, 1), :] = top[g, i] * SCALE + jnp.log(total)
        return carry

    lax.fori_loop(0, Q_HEADS, finish, 0)

    def drain(i, carry):
        row = i // KV_HEADS
        g = lax.rem(i, KV_HEADS)
        moved(0, g, 1, row, other).wait_send()

        @pl.when(g == 0)
        def _():
            moved_seg(0, 1, row, other).wait_send()

        return carry

    lax.fori_loop(0, 16 * KV_HEADS, drain, 0)


def on_device(queries, key_rows, value_rows, segments):
    return pl.pallas_call(
        kernel,
        out_shape=(
            jax.ShapeDtypeStruct((TOK, Q_HEADS * HEAD_DIM), jnp.bfloat16),
            jax.ShapeDtypeStruct((Q_HEADS, TOK), jnp.float32),
        ),
        in_specs=[pl.BlockSpec(memory_space=pl.ANY)] * 4,
        out_specs=(pl.BlockSpec(memory_space=pltpu.VMEM), pl.BlockSpec(memory_space=pltpu.VMEM)),
        scratch_shapes=[
            pltpu.VMEM((SLOTS, KV_HEADS, 2, TOK, HEAD_DIM), jnp.bfloat16),
            pltpu.VMEM((SLOTS, 1, TOK), jnp.int32),
            pltpu.VMEM((TOK, Q_HEADS * HEAD_DIM), jnp.bfloat16),
            pltpu.VMEM((KV_HEADS, GROUP, 2 * HEAD_DIM, TOK), jnp.bfloat16),
            pltpu.VMEM((KV_HEADS, GROUP, HEAD_DIM + ONES, TOK), jnp.float32),
            pltpu.VMEM((KV_HEADS, GROUP, 1, TOK), jnp.float32),
            pltpu.SemaphoreType.DMA((2 * KV_HEADS + 2,)),
            pltpu.SemaphoreType.DMA((SLOTS, KV_HEADS)),
            pltpu.SemaphoreType.DMA((16, KV_HEADS)),
            pltpu.SemaphoreType.DMA((SLOTS,)),
            pltpu.SemaphoreType.DMA((16,)),
        ],
        compiler_params=pltpu.CompilerParams(
            collective_id=0, has_side_effects=True, vmem_limit_bytes=60 * 1024 * 1024),
    )(queries, key_rows, value_rows, segments.reshape(1, TOK))


def solution(mesh):
    split = Mesh(mesh.devices.reshape(mesh.shape["grp"], NX, NZ, 2), GRP_SEQ)
    rows = P(GRP_SEQ, None)
    return jax.shard_map(
        on_device,
        mesh=split,
        in_specs=(rows, rows, rows, P(GRP_SEQ)),
        out_specs=(rows, P(None, GRP_SEQ)),
        check_vma=False,
    )
```

```python
import math

import jax
import jax.numpy as jnp
from jax import lax
from jax.experimental import pallas as pl
from jax.experimental.pallas import tpu as pltpu
from jax.sharding import Mesh
from jax.sharding import PartitionSpec as P

Q_HEADS = 16
KV_HEADS = 4
GROUP = Q_HEADS // KV_HEADS
HEAD_DIM = 128
WINDOW = 4096
TOK = 256
GRP_SEQ = ("grp", "seq_0", "seq_1", "seq_2")
NX, NZ = 4, 8
CHIPS = 128
REACH = WINDOW // (2 * TOK)
SLOTS = 2 * REACH + 1
FWD = 3
BACK = REACH - 1 - FWD
ONES = 16
NEG = -1e30
BIG = -(2.0**100)
SCALE = 1.0 / math.sqrt(HEAD_DIM)
LOG2 = SCALE * math.log2(math.e)
MESH = pl.DeviceIdType.MESH


def kernel(q_hbm, k_hbm, v_hbm, seg_hbm, out_ref, lse_ref, kv, seg, qv, qt, acc, top, bias, score, load_sem, recv_sem, send_sem, seg_recv, seg_send):
    y, x, z, core = (lax.axis_index(a) for a in GRP_SEQ)
    chip = (y * NX + x) * NZ + z

    def at(c, k):
        c = lax.rem(c + CHIPS, CHIPS)
        return (c // (NX * NZ), lax.rem(c // NZ, NX), lax.rem(c, NZ), k)

    ahead, behind = at(chip + 1, core), at(chip - 1, core)
    far, near = at(chip + REACH, core), at(chip - REACH, core)
    other = at(chip, 1 - core)

    loads = []
    for g in range(KV_HEADS):
        cols = pl.ds(g * HEAD_DIM, HEAD_DIM)
        loads.append(pltpu.make_async_copy(k_hbm.at[:, cols], kv.at[0, g, 0], load_sem.at[2 * g]))
        loads.append(pltpu.make_async_copy(v_hbm.at[:, cols], kv.at[0, g, 1], load_sem.at[2 * g + 1]))
    load_seg = pltpu.make_async_copy(seg_hbm, seg.at[0], load_sem.at[2 * KV_HEADS])
    load_q = pltpu.make_async_copy(q_hbm, qv, load_sem.at[2 * KV_HEADS + 1])
    load_seg.start()
    for copy in loads:
        copy.start()
    load_q.start()

    barrier = pltpu.get_barrier_semaphore()
    for peer in (ahead, behind, far, near, other):
        pl.semaphore_signal(barrier, inc=1, device_id=peer, device_id_type=MESH)
    pl.semaphore_wait(barrier, 5)

    def moved(src, g, dst, row, peer):
        return pltpu.make_async_remote_copy(
            src_ref=kv.at[src, g], dst_ref=kv.at[dst, g], send_sem=send_sem.at[row, g],
            recv_sem=recv_sem.at[dst, g], device_id=peer, device_id_type=MESH)

    def moved_seg(src, dst, row, peer):
        return pltpu.make_async_remote_copy(
            src_ref=seg.at[src], dst_ref=seg.at[dst], send_sem=seg_send.at[row],
            recv_sem=seg_recv.at[dst], device_id=peer, device_id_type=MESH)

    def send(src, g, dst, row, peer):
        @pl.when(g == 0)
        def _():
            moved_seg(src, dst, row, peer).start()

        moved(src, g, dst, row, peer).start()

    def arrive(slot, g):
        @pl.when(g == 0)
        def _():
            moved_seg(slot, slot, 0, other).wait_recv()

        moved(slot, g, slot, 0, other).wait_recv()

    def share(j, g):
        t = j - core
        send(j, g, REACH + 1 + t, 8 + t, other)

    load_seg.wait()
    for g in range(KV_HEADS):
        loads[2 * g].wait()
        loads[2 * g + 1].wait()
        send(0, g, REACH, 7, far)

        @pl.when(z != NZ - 1)
        def _():
            send(0, g, 1, 0, ahead)

        @pl.when(core == 0)
        def _():
            share(0, g)

    load_q.wait()

    mine = seg[0]
    q_row = lax.broadcasted_iota(jnp.int32, (1, TOK), 1)
    q_first = mine == mine[:, :1]
    sub = lax.broadcasted_iota(jnp.int32, (HEAD_DIM, TOK), 0)
    marks = jnp.where(sub == 0, 1.0, jnp.where(sub == 1, jnp.where(q_first, 0.0, 1.0), 0.0)).astype(jnp.bfloat16)

    def turn(h, carry):
        g, i = h // GROUP, lax.rem(h, GROUP)
        qt[g, i, :HEAD_DIM] = qv[:, pl.ds(pl.multiple_of(h * HEAD_DIM, HEAD_DIM), HEAD_DIM)].T
        qt[g, i, HEAD_DIM:] = marks
        return carry

    mine_col = jnp.broadcast_to(mine.astype(jnp.float32), (HEAD_DIM, TOK)).T
    mine_col = jnp.concatenate([mine_col, mine_col], axis=1)
    key_pos = lax.broadcasted_iota(jnp.int32, (TOK, TOK), 0)
    q_pos = lax.broadcasted_iota(jnp.int32, (TOK, TOK), 1)
    same = mine_col == jnp.broadcast_to(mine.astype(jnp.float32), (TOK, TOK))
    bias[...] = jnp.where(same & (key_pos <= q_pos), 0.0, NEG)
    lane = lax.broadcasted_iota(jnp.int32, (TOK, HEAD_DIM), 1)
    key_row = lax.broadcasted_iota(jnp.int32, (TOK, HEAD_DIM), 0)

    def keys_of(slot, g):
        back = jnp.where(slot <= REACH, 2 * slot, 2 * (slot - REACH) - 1)
        before = jnp.sum(jnp.where(seg[slot] < mine[:, :1], 1.0, 0.0), axis=1, keepdims=True).astype(jnp.int32)
        before = jnp.maximum(before, jnp.where(2 * chip + core < back, TOK, 0))
        closed = jnp.where(key_row < before, BIG, 0.0)
        columns = jnp.where(lane == 0, closed, jnp.where(lane == 1, BIG, 0.0)).astype(jnp.bfloat16)
        return jnp.concatenate([kv[slot, g, 0], columns], axis=1)

    def values_of(slots, g):
        values = jnp.concatenate([kv[slot, g, 1].T for slot in slots], axis=1)
        return jnp.concatenate([values, jnp.ones((ONES, TOK * len(slots)), jnp.bfloat16)], axis=0)

    def first_blocks(g):
        own, old, values = kv[0, g, 0], keys_of(REACH, g), values_of((0, REACH), g)

        causal = key_pos <= q_pos

        def scores_of(i):
            s_own = jnp.dot(own, qt[g, i, :HEAD_DIM], preferred_element_type=jnp.float32)
            s_old = jnp.dot(old, qt[g, i], preferred_element_type=jnp.float32)
            s = jnp.where(causal, s_own + bias[...], s_old)
            score[i, :TOK] = s
            return jnp.max(s, axis=0, keepdims=True)

        maxima = [scores_of(0)]
        for i in range(GROUP):
            if i + 1 < GROUP:
                maxima.append(scores_of(i + 1))
            m = maxima[i]
            p = jnp.exp2(score[i, :TOK] * LOG2 - m * LOG2)
            p = jnp.concatenate([jnp.where(causal, p, 0.0), jnp.where(causal, 0.0, p)], axis=0).astype(jnp.bfloat16)
            acc[g, i] = jnp.dot(values, p, preferred_element_type=jnp.float32)
        for i in range(GROUP):
            top[g, i] = maxima[i]

    def attend(slots, g):
        keys = jnp.concatenate([keys_of(slot, g) for slot in slots], axis=0)
        values = values_of(slots, g)
        old = [top[g, i] for i in range(GROUP)]

        length = TOK * len(slots)

        def scores_of(i):
            s = jnp.dot(keys, qt[g, i], preferred_element_type=jnp.float32)
            score[i, :length] = s
            return jnp.maximum(old[i], jnp.max(s, axis=0, keepdims=True))

        maxima = [scores_of(0)]
        for i in range(GROUP):
            if i + 1 < GROUP:
                maxima.append(scores_of(i + 1))
            m = maxima[i]
            w = jnp.exp2(score[i, :length] * LOG2 - m * LOG2).astype(jnp.bfloat16)
            update = jnp.dot(values, w, preferred_element_type=jnp.float32)
            acc[g, i] = acc[g, i] * jnp.exp2((old[i] - m) * LOG2) + update
        for i in range(GROUP):
            top[g, i] = maxima[i]

    lag = jnp.where(z == 0, 5, jnp.where(z == 1, 3, 2))

    def tick(t, carry):
        @pl.when(t < KV_HEADS)
        def _():
            arrive(REACH, t)
            send(REACH, t, REACH - 1, 3, behind)

            @pl.when(core == 1)
            def _():
                share(REACH, t)

        @pl.when((t == KV_HEADS - 1) & (z == NZ - 1))
        def _():
            for g in range(KV_HEADS):
                send(0, g, 1, 0, ahead)

        b = t - 1

        @pl.when((b >= 0) & (b < BACK * KV_HEADS))
        def _():
            j, g = REACH - 1 - b // KV_HEADS, lax.rem(b, KV_HEADS)
            arrive(j, g)

            @pl.when(j > FWD + 1)
            def _():
                send(j, g, j - 1, 3 + REACH - j, behind)

            share(j, g)

        f = t - lag

        @pl.when((f >= 0) & (f < FWD * KV_HEADS))
        def _():
            j, g = 1 + f // KV_HEADS, lax.rem(f, KV_HEADS)
            arrive(j, g)

            @pl.when(j < FWD)
            def _():
                send(j, g, j + 1, j, ahead)

            share(j, g)

        @pl.when(t < KV_HEADS)
        def _():
            lax.fori_loop(t * GROUP, (t + 1) * GROUP, turn, 0)
            first_blocks(t)

        def source(r, carry):
            u = t - jnp.where(r == 0, 2, lag + 1)
            v = jnp.maximum(u, 0)
            j = jnp.where(r == 0, REACH - 1 - v // KV_HEADS, 1 + v // KV_HEADS)
            g = lax.rem(v, KV_HEADS)

            @pl.when((u >= 0) & (u < jnp.where(r == 0, BACK, FWD) * KV_HEADS))
            def _():
                arrive(REACH + j + core, g)
                attend((j, REACH + j + core), g)

            return carry

        @pl.when((t >= KV_HEADS) & (t < 2 * KV_HEADS))
        def _():
            slot = 2 * REACH - (REACH - 1) * core
            arrive(slot, t - KV_HEADS)
            attend((slot,), t - KV_HEADS)

        lax.fori_loop(0, 2, source, 0)
        return carry

    lax.fori_loop(0, BACK * KV_HEADS + 2, tick, 0)

    def finish(h, carry):
        g, i = h // GROUP, lax.rem(h, GROUP)
        total = acc[g, i, HEAD_DIM:HEAD_DIM + 1, :]
        part = acc[g, i, :HEAD_DIM, :] / total
        out_ref[:, pl.ds(pl.multiple_of(h * HEAD_DIM, HEAD_DIM), HEAD_DIM)] = part.T.astype(jnp.bfloat16)
        lse_ref[pl.ds(h, 1), :] = top[g, i] * SCALE + jnp.log(total)
        return carry

    lax.fori_loop(0, Q_HEADS, finish, 0)

    def drain(i, carry):
        row = i // KV_HEADS
        g = lax.rem(i, KV_HEADS)
        moved(0, g, 1, row, other).wait_send()

        @pl.when(g == 0)
        def _():
            moved_seg(0, 1, row, other).wait_send()

        return carry

    lax.fori_loop(0, 16 * KV_HEADS, drain, 0)


def on_device(queries, key_rows, value_rows, segments):
    return pl.pallas_call(
        kernel,
        out_shape=(
            jax.ShapeDtypeStruct((TOK, Q_HEADS * HEAD_DIM), jnp.bfloat16),
            jax.ShapeDtypeStruct((Q_HEADS, TOK), jnp.float32),
        ),
        in_specs=[pl.BlockSpec(memory_space=pl.ANY)] * 4,
        out_specs=(pl.BlockSpec(memory_space=pltpu.VMEM), pl.BlockSpec(memory_space=pltpu.VMEM)),
        scratch_shapes=[
            pltpu.VMEM((SLOTS, KV_HEADS, 2, TOK, HEAD_DIM), jnp.bfloat16),
            pltpu.VMEM((SLOTS, 1, TOK), jnp.int32),
            pltpu.VMEM((TOK, Q_HEADS * HEAD_DIM), jnp.bfloat16),
            pltpu.VMEM((KV_HEADS, GROUP, 2 * HEAD_DIM, TOK), jnp.bfloat16),
            pltpu.VMEM((KV_HEADS, GROUP, HEAD_DIM + ONES, TOK), jnp.float32),
            pltpu.VMEM((KV_HEADS, GROUP, 1, TOK), jnp.float32),
            pltpu.VMEM((TOK, TOK), jnp.float32),
            pltpu.VMEM((4, 2 * TOK, TOK), jnp.float32),
            pltpu.SemaphoreType.DMA((2 * KV_HEADS + 2,)),
            pltpu.SemaphoreType.DMA((SLOTS, KV_HEADS)),
            pltpu.SemaphoreType.DMA((16, KV_HEADS)),
            pltpu.SemaphoreType.DMA((SLOTS,)),
            pltpu.SemaphoreType.DMA((16,)),
        ],
        compiler_params=pltpu.CompilerParams(
            collective_id=0, has_side_effects=True, vmem_limit_bytes=30 * 1024 * 1024),
    )(*(pltpu.with_memory_space_constraint(a, pltpu.HBM) for a in (queries, key_rows, value_rows)), segments.reshape(1, TOK))


def solution(mesh):
    split = Mesh(mesh.devices.reshape(mesh.shape["grp"], NX, NZ, 2), GRP_SEQ)
    rows = P(GRP_SEQ, None)
    return jax.shard_map(
        on_device,
        mesh=split,
        in_specs=(rows, rows, rows, P(GRP_SEQ)),
        out_specs=(rows, P(None, GRP_SEQ)),
        check_vma=False,
    )
```

```python
import math

import jax
import jax.numpy as jnp
from jax import lax
from jax.experimental import pallas as pl
from jax.experimental.pallas import tpu as pltpu
from jax.sharding import Mesh
from jax.sharding import PartitionSpec as P

Q_HEADS = 16
KV_HEADS = 4
GROUP = Q_HEADS // KV_HEADS
HEAD_DIM = 128
WINDOW = 4096
TOK = 256
GRP_SEQ = ("grp", "seq_0", "seq_1", "seq_2")
NX, NZ = 4, 8
CHIPS = 128
REACH = WINDOW // (2 * TOK)
SLOTS = 2 * REACH + 1
FWD = 3
BACK = REACH - 1 - FWD
ONES = 16
NEG = -1e30
BIG = -(2.0**100)
SCALE = 1.0 / math.sqrt(HEAD_DIM)
LOG2 = SCALE * math.log2(math.e)
MESH = pl.DeviceIdType.MESH


def kernel(q_hbm, k_hbm, v_hbm, seg_hbm, out_ref, lse_ref, kv, seg, qv, qt, acc, top, bias, score, load_sem, recv_sem, send_sem, seg_recv, seg_send):
    y, x, z, core = (lax.axis_index(a) for a in GRP_SEQ)
    chip = (y * NX + x) * NZ + z

    def at(c, k):
        c = lax.rem(c + CHIPS, CHIPS)
        return (c // (NX * NZ), lax.rem(c // NZ, NX), lax.rem(c, NZ), k)

    ahead, behind = at(chip + 1, core), at(chip - 1, core)
    far, near = at(chip + REACH, core), at(chip - REACH, core)
    other = at(chip, 1 - core)

    first, last = z == 0, z == NZ - 1

    def real(c, j):
        c = lax.rem(c + CHIPS, CHIPS)
        return (c >= REACH) | (j <= c)

    def live(c, j):
        return real(c, j) | (j >= lax.rem(c + CHIPS, CHIPS) + REACH - 2)

    def sent_ahead(j):
        return ((j < FWD) | ((j == FWD) & (z == NZ - 2))) & live(chip, j) & live(chip + 1, j + 1)

    def sent_behind(j):
        return (j > FWD + 1) & live(chip, j) & live(chip - 1, j - 1) & jnp.logical_not(first & (j == FWD + 2))

    loads = []
    for g in range(KV_HEADS):
        cols = pl.ds(g * HEAD_DIM, HEAD_DIM)
        loads.append(pltpu.make_async_copy(k_hbm.at[:, cols], kv.at[0, g, 0], load_sem.at[2 * g]))
        loads.append(pltpu.make_async_copy(v_hbm.at[:, cols], kv.at[0, g, 1], load_sem.at[2 * g + 1]))
    load_seg = pltpu.make_async_copy(seg_hbm, seg.at[0], load_sem.at[2 * KV_HEADS])
    load_q = pltpu.make_async_copy(q_hbm, qv, load_sem.at[2 * KV_HEADS + 1])
    load_seg.start()
    for copy in loads:
        copy.start()
    load_q.start()

    barrier = pltpu.get_barrier_semaphore()
    for peer in (ahead, behind, far, near, other):
        pl.semaphore_signal(barrier, inc=1, device_id=peer, device_id_type=MESH)
    pl.semaphore_wait(barrier, 5)

    def moved(src, g, dst, row, peer):
        return pltpu.make_async_remote_copy(
            src_ref=kv.at[src, g], dst_ref=kv.at[dst, g], send_sem=send_sem.at[row, g],
            recv_sem=recv_sem.at[dst, g], device_id=peer, device_id_type=MESH)

    def moved_seg(src, dst, row, peer):
        return pltpu.make_async_remote_copy(
            src_ref=seg.at[src], dst_ref=seg.at[dst], send_sem=seg_send.at[row],
            recv_sem=seg_recv.at[dst], device_id=peer, device_id_type=MESH)

    def send(src, g, dst, row, peer):
        @pl.when(g == 0)
        def _():
            moved_seg(src, dst, row, peer).start()

        moved(src, g, dst, row, peer).start()

    def arrive(slot, g):
        @pl.when(g == 0)
        def _():
            moved_seg(slot, slot, 0, other).wait_recv()

        moved(slot, g, slot, 0, other).wait_recv()

    def share(j, g):
        t = j - core
        send(j, g, REACH + 1 + t, 9 + t, other)

    load_seg.wait()
    for g in range(KV_HEADS):
        loads[2 * g].wait()
        loads[2 * g + 1].wait()

        @pl.when(live(chip + REACH, REACH))
        def _():
            send(0, g, REACH, 8, far)

        @pl.when(sent_ahead(0) & jnp.logical_not(last))
        def _():
            send(0, g, 1, 0, ahead)

        @pl.when(core == 0)
        def _():
            share(0, g)

    load_q.wait()

    mine = seg[0]
    q_row = lax.broadcasted_iota(jnp.int32, (1, TOK), 1)
    q_first = mine == mine[:, :1]
    sub = lax.broadcasted_iota(jnp.int32, (HEAD_DIM, TOK), 0)
    marks = jnp.where(sub == 0, 1.0, jnp.where(sub == 1, jnp.where(q_first, 0.0, 1.0), 0.0)).astype(jnp.bfloat16)

    def turn(h, carry):
        g, i = h // GROUP, lax.rem(h, GROUP)
        qt[g, i, :HEAD_DIM] = qv[:, pl.ds(pl.multiple_of(h * HEAD_DIM, HEAD_DIM), HEAD_DIM)].T
        qt[g, i, HEAD_DIM:] = marks
        return carry

    mine_col = jnp.broadcast_to(mine.astype(jnp.float32), (HEAD_DIM, TOK)).T
    mine_col = jnp.concatenate([mine_col, mine_col], axis=1)
    key_pos = lax.broadcasted_iota(jnp.int32, (TOK, TOK), 0)
    q_pos = lax.broadcasted_iota(jnp.int32, (TOK, TOK), 1)
    same = mine_col == jnp.broadcast_to(mine.astype(jnp.float32), (TOK, TOK))
    bias[...] = jnp.where(same & (key_pos <= q_pos), 0.0, NEG)
    lane = lax.broadcasted_iota(jnp.int32, (TOK, HEAD_DIM), 1)
    key_row = lax.broadcasted_iota(jnp.int32, (TOK, HEAD_DIM), 0)

    def keys_of(slot, g, back):
        before = jnp.sum(jnp.where(seg[slot] < mine[:, :1], 1.0, 0.0), axis=1, keepdims=True).astype(jnp.int32)
        before = jnp.maximum(before, jnp.where(2 * chip + core < back, TOK, 0))
        closed = jnp.where(key_row < before, BIG, 0.0)
        columns = jnp.where(lane == 0, closed, jnp.where(lane == 1, BIG, 0.0)).astype(jnp.bfloat16)
        return jnp.concatenate([kv[slot, g, 0], columns], axis=1)

    def values_of(slots, g):
        values = jnp.concatenate([kv[slot, g, 1].T for slot in slots], axis=1)
        return jnp.concatenate([values, jnp.ones((ONES, TOK * len(slots)), jnp.bfloat16)], axis=0)

    def first_blocks(g):
        slot = jnp.where(real(chip, REACH), REACH, 0)
        own, old, values = kv[0, g, 0], keys_of(slot, g, 2 * REACH), values_of((0, slot), g)

        causal = key_pos <= q_pos

        def scores_of(i):
            s_own = jnp.dot(own, qt[g, i, :HEAD_DIM], preferred_element_type=jnp.float32)
            s_old = jnp.dot(old, qt[g, i], preferred_element_type=jnp.float32)
            s = jnp.where(causal, s_own + bias[...], s_old)
            score[i, :TOK] = s
            return jnp.max(s, axis=0, keepdims=True)

        maxima = [scores_of(0)]
        for i in range(GROUP):
            if i + 1 < GROUP:
                maxima.append(scores_of(i + 1))
            m = maxima[i]
            p = jnp.exp2(score[i, :TOK] * LOG2 - m * LOG2)
            p = jnp.concatenate([jnp.where(causal, p, 0.0), jnp.where(causal, 0.0, p)], axis=0).astype(jnp.bfloat16)
            acc[g, i] = jnp.dot(values, p, preferred_element_type=jnp.float32)
        for i in range(GROUP):
            top[g, i] = maxima[i]

    def attend(slots, g):
        keys = jnp.concatenate([keys_of(slot, g, jnp.where(slot <= REACH, 2 * slot, 2 * (slot - REACH) - 1)) for slot in slots], axis=0)
        values = values_of(slots, g)
        old = [top[g, i] for i in range(GROUP)]

        length = TOK * len(slots)

        def scores_of(i):
            s = jnp.dot(keys, qt[g, i], preferred_element_type=jnp.float32)
            score[i, :length] = s
            return jnp.maximum(old[i], jnp.max(s, axis=0, keepdims=True))

        maxima = [scores_of(0)]
        for i in range(GROUP):
            if i + 1 < GROUP:
                maxima.append(scores_of(i + 1))
            m = maxima[i]
            w = jnp.exp2(score[i, :length] * LOG2 - m * LOG2).astype(jnp.bfloat16)
            update = jnp.dot(values, w, preferred_element_type=jnp.float32)
            acc[g, i] = acc[g, i] * jnp.exp2((old[i] - m) * LOG2) + update
        for i in range(GROUP):
            top[g, i] = maxima[i]

    lag = jnp.where(first, 6, jnp.where(z == 1, 3, 1))

    def tick(t, carry):
        @pl.when((t < KV_HEADS) & live(chip, REACH))
        def _():
            arrive(REACH, t)

            @pl.when(sent_behind(REACH))
            def _():
                send(REACH, t, REACH - 1, 4, behind)

            @pl.when((core == 1) & real(chip, REACH))
            def _():
                share(REACH, t)

        b = t - 1
        j_b, g_b = REACH - 1 - jnp.maximum(b, 0) // KV_HEADS, lax.rem(b + KV_HEADS, KV_HEADS)

        @pl.when((b >= 0) & (b < BACK * KV_HEADS) & live(chip, j_b) & jnp.logical_not(last & (j_b == FWD + 1)))
        def _():
            arrive(j_b, g_b)

            @pl.when(sent_behind(j_b))
            def _():
                send(j_b, g_b, j_b - 1, 4 + REACH - j_b, behind)

            @pl.when(real(chip, j_b))
            def _():
                share(j_b, g_b)

        k = t - 2

        @pl.when((k >= 0) & (k < 2) & last & sent_ahead(0))
        def _():
            send(0, 2 * k, 1, 0, ahead)
            send(0, 2 * k + 1, 1, 0, ahead)

        r = t - 4
        j_r, g_r = 1 + jnp.maximum(r, 0) // KV_HEADS, lax.rem(r + KV_HEADS, KV_HEADS)

        @pl.when((r >= 0) & (r < (FWD - 1) * KV_HEADS) & last & sent_ahead(j_r))
        def _():
            send(j_r, g_r, j_r + 1, j_r, ahead)

        f = t - lag
        j_f, g_f = 1 + jnp.maximum(f, 0) // KV_HEADS, lax.rem(f + 2 * KV_HEADS, KV_HEADS)

        @pl.when((f >= 0) & ((j_f <= FWD) | ((j_f == FWD + 1) & last)) & live(chip, j_f))
        def _():
            arrive(j_f, g_f)

            @pl.when(sent_ahead(j_f) & jnp.logical_not(last))
            def _():
                send(j_f, g_f, j_f + 1, j_f, ahead)

            share(j_f, g_f)

        @pl.when(t < KV_HEADS)
        def _():
            lax.fori_loop(t * GROUP, (t + 1) * GROUP, turn, 0)
            first_blocks(t)

        def source(r, carry):
            u = t - jnp.where(r == 0, 2, lag + 1)
            v = jnp.maximum(u, 0)
            j = jnp.where(r == 0, REACH - 1 - v // KV_HEADS, 1 + v // KV_HEADS)
            g = lax.rem(v, KV_HEADS)
            turned = last & (j == FWD + 1)
            mine_here = jnp.where(r == 0, (j > FWD) & jnp.logical_not(turned), (j <= FWD) | turned)

            @pl.when((u >= 0) & mine_here & real(chip, j))
            def _():
                arrive(REACH + j + core, g)
                attend((j, REACH + j + core), g)

            return carry

        @pl.when((t >= KV_HEADS) & (t < 2 * KV_HEADS) & ((core == 1) | real(chip, REACH)))
        def _():
            slot = 2 * REACH - (REACH - 1) * core
            arrive(slot, t - KV_HEADS)
            attend((slot,), t - KV_HEADS)

        lax.fori_loop(0, 2, source, 0)
        return carry

    lax.fori_loop(0, BACK * KV_HEADS + 3, tick, 0)

    def finish(h, carry):
        g, i = h // GROUP, lax.rem(h, GROUP)
        total = acc[g, i, HEAD_DIM:HEAD_DIM + 1, :]
        part = acc[g, i, :HEAD_DIM, :] / total
        out_ref[:, pl.ds(pl.multiple_of(h * HEAD_DIM, HEAD_DIM), HEAD_DIM)] = part.T.astype(jnp.bfloat16)
        lse_ref[pl.ds(h, 1), :] = top[g, i] * SCALE + jnp.log(total)
        return carry

    lax.fori_loop(0, Q_HEADS, finish, 0)

    def drain(i, carry):
        row, g = i // KV_HEADS, lax.rem(i, KV_HEADS)
        sent = jnp.where(row < 4, sent_ahead(row), jnp.where(row < 8, sent_behind(REACH + 4 - row), jnp.where(
            row == 8, live(chip + REACH, REACH), real(chip, row - 9 + core))))

        @pl.when(sent)
        def _():
            moved(0, g, 1, row, other).wait_send()

            @pl.when(g == 0)
            def _():
                moved_seg(0, 1, row, other).wait_send()

        return carry

    lax.fori_loop(0, 17 * KV_HEADS, drain, 0)


def on_device(queries, key_rows, value_rows, segments):
    return pl.pallas_call(
        kernel,
        out_shape=(
            jax.ShapeDtypeStruct((TOK, Q_HEADS * HEAD_DIM), jnp.bfloat16),
            jax.ShapeDtypeStruct((Q_HEADS, TOK), jnp.float32),
        ),
        in_specs=[pl.BlockSpec(memory_space=pl.ANY)] * 4,
        out_specs=(pl.BlockSpec(memory_space=pltpu.VMEM), pl.BlockSpec(memory_space=pltpu.VMEM)),
        scratch_shapes=[
            pltpu.VMEM((SLOTS, KV_HEADS, 2, TOK, HEAD_DIM), jnp.bfloat16),
            pltpu.VMEM((SLOTS, 1, TOK), jnp.int32),
            pltpu.VMEM((TOK, Q_HEADS * HEAD_DIM), jnp.bfloat16),
            pltpu.VMEM((KV_HEADS, GROUP, 2 * HEAD_DIM, TOK), jnp.bfloat16),
            pltpu.VMEM((KV_HEADS, GROUP, HEAD_DIM + ONES, TOK), jnp.float32),
            pltpu.VMEM((KV_HEADS, GROUP, 1, TOK), jnp.float32),
            pltpu.VMEM((TOK, TOK), jnp.float32),
            pltpu.VMEM((4, 2 * TOK, TOK), jnp.float32),
            pltpu.SemaphoreType.DMA((2 * KV_HEADS + 2,)),
            pltpu.SemaphoreType.DMA((SLOTS, KV_HEADS)),
            pltpu.SemaphoreType.DMA((17, KV_HEADS)),
            pltpu.SemaphoreType.DMA((SLOTS,)),
            pltpu.SemaphoreType.DMA((17,)),
        ],
        compiler_params=pltpu.CompilerParams(
            collective_id=0, has_side_effects=True, vmem_limit_bytes=30 * 1024 * 1024),
    )(*(pltpu.with_memory_space_constraint(a, pltpu.HBM) for a in (queries, key_rows, value_rows, segments.reshape(1, TOK))))


def solution(mesh):
    split = Mesh(mesh.devices.reshape(mesh.shape["grp"], NX, NZ, 2), GRP_SEQ)
    rows = P(GRP_SEQ, None)
    return jax.shard_map(
        on_device,
        mesh=split,
        in_specs=(rows, rows, rows, P(GRP_SEQ)),
        out_specs=(rows, P(None, GRP_SEQ)),
        check_vma=False,
    )
```

```python
import math

import jax
import jax.numpy as jnp
from jax import lax
from jax.experimental import pallas as pl
from jax.experimental.pallas import tpu as pltpu
from jax.sharding import Mesh
from jax.sharding import PartitionSpec as P

Q_HEADS = 16
KV_HEADS = 4
GROUP = Q_HEADS // KV_HEADS
HEAD_DIM = 128
WINDOW = 4096
TOK = 256
GRP_SEQ = ("grp", "seq_0", "seq_1", "seq_2")
NX, NZ = 4, 8
CHIPS = 128
REACH = WINDOW // (2 * TOK)
SLOTS = 2 * REACH + 1
FWD = 3
BACK = REACH - 1 - FWD
ONES = 16
NEG = -1e30
BIG = -(2.0**100)
SCALE = 1.0 / math.sqrt(HEAD_DIM)
LOG2 = SCALE * math.log2(math.e)
MESH = pl.DeviceIdType.MESH


def kernel(q_hbm, k_hbm, v_hbm, seg_hbm, out_ref, lse_ref, kv, seg, qv, qt, acc, top, bias, score, load_sem, recv_sem, send_sem, seg_recv, seg_send):
    y, x, z, core = (lax.axis_index(a) for a in GRP_SEQ)
    chip = (y * NX + x) * NZ + z

    def at(c, k):
        c = lax.rem(c + CHIPS, CHIPS)
        return (c // (NX * NZ), lax.rem(c // NZ, NX), lax.rem(c, NZ), k)

    ahead, behind = at(chip + 1, core), at(chip - 1, core)
    far, near = at(chip + REACH, core), at(chip - REACH, core)
    other = at(chip, 1 - core)

    first, last = z == 0, z == NZ - 1

    def real(c, j):
        c = lax.rem(c + CHIPS, CHIPS)
        return (c >= REACH) | (j <= c)

    def live(c, j):
        return real(c, j) | (j >= lax.rem(c + CHIPS, CHIPS) + REACH - 2)

    def sent_ahead(j):
        return ((j < FWD) | ((j == FWD) & (z == NZ - 2))) & live(chip, j) & live(chip + 1, j + 1)

    def sent_behind(j):
        return (j > FWD + 1) & live(chip, j) & live(chip - 1, j - 1) & jnp.logical_not(first & (j == FWD + 2))

    loads = []
    for g in range(KV_HEADS):
        cols = pl.ds(g * HEAD_DIM, HEAD_DIM)
        loads.append(pltpu.make_async_copy(k_hbm.at[:, cols], kv.at[0, g, 0], load_sem.at[2 * g]))
        loads.append(pltpu.make_async_copy(v_hbm.at[:, cols], kv.at[0, g, 1], load_sem.at[2 * g + 1]))
    load_seg = pltpu.make_async_copy(seg_hbm, seg.at[0], load_sem.at[2 * KV_HEADS])
    load_q = pltpu.make_async_copy(q_hbm, qv, load_sem.at[2 * KV_HEADS + 1])
    load_seg.start()
    for copy in loads:
        copy.start()
    load_q.start()

    barrier = pltpu.get_barrier_semaphore()
    for peer in (ahead, behind, far, near, other):
        pl.semaphore_signal(barrier, inc=1, device_id=peer, device_id_type=MESH)
    pl.semaphore_wait(barrier, 5)

    def moved(src, g, dst, row, peer):
        return pltpu.make_async_remote_copy(
            src_ref=kv.at[src, g], dst_ref=kv.at[dst, g], send_sem=send_sem.at[row, g],
            recv_sem=recv_sem.at[dst, g], device_id=peer, device_id_type=MESH)

    def moved_seg(src, dst, row, peer):
        return pltpu.make_async_remote_copy(
            src_ref=seg.at[src], dst_ref=seg.at[dst], send_sem=seg_send.at[row],
            recv_sem=seg_recv.at[dst], device_id=peer, device_id_type=MESH)

    def send(src, g, dst, row, peer):
        @pl.when(g == 0)
        def _():
            moved_seg(src, dst, row, peer).start()

        moved(src, g, dst, row, peer).start()

    def arrive(slot, g):
        @pl.when(g == 0)
        def _():
            moved_seg(slot, slot, 0, other).wait_recv()

        moved(slot, g, slot, 0, other).wait_recv()

    def share(j, g):
        t = j - core
        send(j, g, REACH + 1 + t, 9 + t, other)

    load_seg.wait()
    for g in range(KV_HEADS):
        loads[2 * g].wait()
        loads[2 * g + 1].wait()

        @pl.when(live(chip + REACH, REACH))
        def _():
            send(0, g, REACH, 8, far)

        @pl.when(sent_ahead(0) & jnp.logical_not(last))
        def _():
            send(0, g, 1, 0, ahead)

        @pl.when(core == 0)
        def _():
            share(0, g)

    load_q.wait()

    mine = seg[0]
    q_row = lax.broadcasted_iota(jnp.int32, (1, TOK), 1)
    q_first = mine == mine[:, :1]
    sub = lax.broadcasted_iota(jnp.int32, (HEAD_DIM, TOK), 0)
    marks = jnp.where(sub == 0, 1.0, jnp.where(sub == 1, jnp.where(q_first, 0.0, 1.0), 0.0)).astype(jnp.bfloat16)

    def turn(h, carry):
        g, i = h // GROUP, lax.rem(h, GROUP)
        qt[g, i, :HEAD_DIM] = qv[:, pl.ds(pl.multiple_of(h * HEAD_DIM, HEAD_DIM), HEAD_DIM)].T
        qt[g, i, HEAD_DIM:] = marks
        return carry

    mine_col = jnp.broadcast_to(mine.astype(jnp.float32), (HEAD_DIM, TOK)).T
    mine_col = jnp.concatenate([mine_col, mine_col], axis=1)
    key_pos = lax.broadcasted_iota(jnp.int32, (TOK, TOK), 0)
    q_pos = lax.broadcasted_iota(jnp.int32, (TOK, TOK), 1)
    same = mine_col == jnp.broadcast_to(mine.astype(jnp.float32), (TOK, TOK))
    bias[...] = jnp.where(same & (key_pos <= q_pos), 0.0, NEG)
    lane = lax.broadcasted_iota(jnp.int32, (TOK, HEAD_DIM), 1)
    key_row = lax.broadcasted_iota(jnp.int32, (TOK, HEAD_DIM), 0)

    def keys_of(slot, g, back):
        before = jnp.sum(jnp.where(seg[slot] < mine[:, :1], 1.0, 0.0), axis=1, keepdims=True).astype(jnp.int32)
        before = jnp.maximum(before, jnp.where(2 * chip + core < back, TOK, 0))
        closed = jnp.where(key_row < before, BIG, 0.0)
        columns = jnp.where(lane == 0, closed, jnp.where(lane == 1, BIG, 0.0)).astype(jnp.bfloat16)
        return jnp.concatenate([kv[slot, g, 0], columns], axis=1)

    def values_of(slots, g):
        values = jnp.concatenate([kv[slot, g, 1].T for slot in slots], axis=1)
        return jnp.concatenate([values, jnp.ones((ONES, TOK * len(slots)), jnp.bfloat16)], axis=0)

    def first_blocks(g):
        slot = jnp.where(real(chip, REACH), REACH, 0)
        own, old, values = kv[0, g, 0], keys_of(slot, g, 2 * REACH), values_of((0, slot), g)

        causal = key_pos <= q_pos

        def scores_of(i):
            s_own = jnp.dot(own, qt[g, i, :HEAD_DIM], preferred_element_type=jnp.float32)
            s_old = jnp.dot(old, qt[g, i], preferred_element_type=jnp.float32)
            s = jnp.where(causal, s_own + bias[...], s_old)
            score[i, :TOK] = s
            return jnp.max(s, axis=0, keepdims=True)

        maxima = [scores_of(0)]
        for i in range(GROUP):
            if i + 1 < GROUP:
                maxima.append(scores_of(i + 1))
            m = maxima[i]
            p = jnp.exp2(score[i, :TOK] * LOG2 - m * LOG2)
            p = jnp.concatenate([jnp.where(causal, p, 0.0), jnp.where(causal, 0.0, p)], axis=0).astype(jnp.bfloat16)
            acc[g, i] = jnp.dot(values, p, preferred_element_type=jnp.float32)
        for i in range(GROUP):
            top[g, i] = maxima[i]

    def attend(slots, g):
        keys = jnp.concatenate([keys_of(slot, g, jnp.where(slot <= REACH, 2 * slot, 2 * (slot - REACH) - 1)) for slot in slots], axis=0)
        values = values_of(slots, g)
        old = [top[g, i] for i in range(GROUP)]

        length = TOK * len(slots)

        def scores_of(i):
            s = jnp.dot(keys, qt[g, i], preferred_element_type=jnp.float32)
            score[i, :length] = s
            return jnp.maximum(old[i], jnp.max(s, axis=0, keepdims=True))

        maxima = [scores_of(0)]
        for i in range(GROUP):
            if i + 1 < GROUP:
                maxima.append(scores_of(i + 1))
            m = maxima[i]
            w = jnp.exp2(score[i, :length] * LOG2 - m * LOG2).astype(jnp.bfloat16)
            update = jnp.dot(values, w, preferred_element_type=jnp.float32)
            acc[g, i] = acc[g, i] * jnp.exp2((old[i] - m) * LOG2) + update
        for i in range(GROUP):
            top[g, i] = maxima[i]

    lag = jnp.where(first, 6, jnp.where(z == 1, 3, 1))

    def drain(rows, shared):
        for row in rows:
            sent = sent_ahead(row) if row < 4 else sent_behind(REACH + 4 - row) if row < 8 else live(chip + REACH, REACH)
            drain_row(row, sent)
        for j in shared:
            drain_row(9 + j - core, real(chip, j))

    def drain_row(row, sent):
        @pl.when(sent)
        def _():
            moved_seg(0, 1, row, other).wait_send()
            for g in range(KV_HEADS):
                moved(0, g, 1, row, other).wait_send()

    def tick(t, carry):
        @pl.when((t < KV_HEADS) & live(chip, REACH))
        def _():
            arrive(REACH, t)

            @pl.when(sent_behind(REACH))
            def _():
                send(REACH, t, REACH - 1, 4, behind)

            @pl.when((core == 1) & real(chip, REACH))
            def _():
                share(REACH, t)

        b = t - 1
        j_b, g_b = REACH - 1 - jnp.maximum(b, 0) // KV_HEADS, lax.rem(b + KV_HEADS, KV_HEADS)

        @pl.when((b >= 0) & (b < BACK * KV_HEADS) & live(chip, j_b) & jnp.logical_not(last & (j_b == FWD + 1)))
        def _():
            arrive(j_b, g_b)

            @pl.when(sent_behind(j_b))
            def _():
                send(j_b, g_b, j_b - 1, 4 + REACH - j_b, behind)

            @pl.when(real(chip, j_b))
            def _():
                share(j_b, g_b)

        k = t - 2

        @pl.when((k >= 0) & (k < 2) & last & sent_ahead(0))
        def _():
            send(0, 2 * k, 1, 0, ahead)
            send(0, 2 * k + 1, 1, 0, ahead)

        r = t - 4
        j_r, g_r = 1 + jnp.maximum(r, 0) // KV_HEADS, lax.rem(r + KV_HEADS, KV_HEADS)

        @pl.when((r >= 0) & (r < (FWD - 1) * KV_HEADS) & last & sent_ahead(j_r))
        def _():
            send(j_r, g_r, j_r + 1, j_r, ahead)

        f = t - lag
        j_f, g_f = 1 + jnp.maximum(f, 0) // KV_HEADS, lax.rem(f + 2 * KV_HEADS, KV_HEADS)

        @pl.when((f >= 0) & ((j_f <= FWD) | ((j_f == FWD + 1) & last)) & live(chip, j_f))
        def _():
            arrive(j_f, g_f)

            @pl.when(sent_ahead(j_f) & jnp.logical_not(last))
            def _():
                send(j_f, g_f, j_f + 1, j_f, ahead)

            share(j_f, g_f)

        @pl.when(t < KV_HEADS)
        def _():
            lax.fori_loop(t * GROUP, (t + 1) * GROUP, turn, 0)
            first_blocks(t)

        def source(r, carry):
            u = t - jnp.where(r == 0, 2, lag + 1)
            v = jnp.maximum(u, 0)
            j = jnp.where(r == 0, REACH - 1 - v // KV_HEADS, 1 + v // KV_HEADS)
            g = lax.rem(v, KV_HEADS)
            turned = last & (j == FWD + 1)
            mine_here = jnp.where(r == 0, (j > FWD) & jnp.logical_not(turned), (j <= FWD) | turned)

            @pl.when((u >= 0) & mine_here & real(chip, j))
            def _():
                arrive(REACH + j + core, g)
                attend((j, REACH + j + core), g)

            return carry

        @pl.when((t >= KV_HEADS) & (t < 2 * KV_HEADS) & ((core == 1) | real(chip, REACH)))
        def _():
            slot = 2 * REACH - (REACH - 1) * core
            arrive(slot, t - KV_HEADS)
            attend((slot,), t - KV_HEADS)

        lax.fori_loop(0, 2, source, 0)

        @pl.when(t == 14)
        def _():
            drain((0, 1, 4, 5, 8), (1, 2, 6, 7))
            drain_row(9 + (REACH - 1) * core, jnp.where(core == 1, real(chip, REACH), chip >= 0))

        return carry

    lax.fori_loop(0, BACK * KV_HEADS + 3, tick, 0)

    def finish(g, carry):
        for i in range(GROUP):
            h = g * GROUP + i
            total = acc[g, i, HEAD_DIM:HEAD_DIM + 1, :]
            part = acc[g, i, :HEAD_DIM, :] / total
            out_ref[:, pl.ds(pl.multiple_of(h * HEAD_DIM, HEAD_DIM), HEAD_DIM)] = part.T.astype(jnp.bfloat16)
            lse_ref[pl.ds(h, 1), :] = top[g, i] * SCALE + jnp.log(total)
        return carry

    lax.fori_loop(0, KV_HEADS, finish, 0)
    drain((2, 3, 6, 7), (3, 4, 5))


def on_device(queries, key_rows, value_rows, segments):
    return pl.pallas_call(
        kernel,
        out_shape=(
            jax.ShapeDtypeStruct((TOK, Q_HEADS * HEAD_DIM), jnp.bfloat16),
            jax.ShapeDtypeStruct((Q_HEADS, TOK), jnp.float32),
        ),
        in_specs=[pl.BlockSpec(memory_space=pl.ANY)] * 4,
        out_specs=(pl.BlockSpec(memory_space=pltpu.VMEM), pl.BlockSpec(memory_space=pltpu.VMEM)),
        scratch_shapes=[
            pltpu.VMEM((SLOTS, KV_HEADS, 2, TOK, HEAD_DIM), jnp.bfloat16),
            pltpu.VMEM((SLOTS, 1, TOK), jnp.int32),
            pltpu.VMEM((TOK, Q_HEADS * HEAD_DIM), jnp.bfloat16),
            pltpu.VMEM((KV_HEADS, GROUP, 2 * HEAD_DIM, TOK), jnp.bfloat16),
            pltpu.VMEM((KV_HEADS, GROUP, HEAD_DIM + ONES, TOK), jnp.float32),
            pltpu.VMEM((KV_HEADS, GROUP, 1, TOK), jnp.float32),
            pltpu.VMEM((TOK, TOK), jnp.float32),
            pltpu.VMEM((4, 2 * TOK, TOK), jnp.float32),
            pltpu.SemaphoreType.DMA((2 * KV_HEADS + 2,)),
            pltpu.SemaphoreType.DMA((SLOTS, KV_HEADS)),
            pltpu.SemaphoreType.DMA((17, KV_HEADS)),
            pltpu.SemaphoreType.DMA((SLOTS,)),
            pltpu.SemaphoreType.DMA((17,)),
        ],
        compiler_params=pltpu.CompilerParams(
            collective_id=0, has_side_effects=True, vmem_limit_bytes=30 * 1024 * 1024),
    )(*(pltpu.with_memory_space_constraint(a, pltpu.HBM) for a in (queries, key_rows, value_rows, segments.reshape(1, TOK))))


def solution(mesh):
    split = Mesh(mesh.devices.reshape(mesh.shape["grp"], NX, NZ, 2), GRP_SEQ)
    rows = P(GRP_SEQ, None)
    return jax.shard_map(
        on_device,
        mesh=split,
        in_specs=(rows, rows, rows, P(GRP_SEQ)),
        out_specs=(rows, P(None, GRP_SEQ)),
        check_vma=False,
    )
```
